32 devices in a mesh: gx: 4 (over y, core), gy: 2 (over x), gz: 4 (over z).
Axes of the slice: x: 2, y: 2, z: 4, core: 2. Of those that a mesh axis runs over, the one named last changes fastest.
Arguments:
- noisy_image: float32 [32, 64, 512], P('gz', 'gy', 'gx'), may hold values from -6 to 6
- fidelity: float32 [32, 64, 512], P('gz', 'gy', 'gx'), may hold values from 0.5 to 8
- primal_u: float32 [32, 64, 512], P('gz', 'gy', 'gx'), may hold values from -6 to 6
- primal_v: float32 [3, 32, 64, 512], P(None, 'gz', 'gy', 'gx'), may hold values from -2 to 2
- dual_p: float32 [3, 32, 64, 512], P(None, 'gz', 'gy', 'gx'), may hold values from -2.5 to 2.5
- dual_q: float32 [6, 32, 64, 512], P(None, 'gz', 'gy', 'gx'), may hold values from -2.5 to 2.5
Outputs:
- denoised: float32 [32, 64, 512], P('gz', 'gy', 'gx')
- vector_field: float32 [3, 32, 64, 512], P(None, 'gz', 'gy', 'gx')
- grad_dual: float32 [3, 32, 64, 512], P(None, 'gz', 'gy', 'gx')
- sym_dual: float32 [6, 32, 64, 512], P(None, 'gz', 'gy', 'gx')
The draws below stay inside these ranges and needn't reach their ends.
All inputs are finite; a program needn't handle non-finite values.
Results may differ from the reference program's by a relative error of at most 0.0001.
Values sent between devices are 32-bit elements; how exact they have to be, the bound alone decides.
A program may use at most 64 MiB of HBM per device.

```python
import math
import jax
import jax.numpy as jnp
from jax import lax

ITERS = 3
NX = 512
NY = 64
NZ = 32


def shard_levels(stream_key, shape, split, smallest, largest):
    def one(dim, shards_of):
        draws = jax.random.uniform(jax.random.fold_in(jax.random.fold_in(stream_key, 6), dim), (shards_of,), jnp.float32, smallest / len(split), largest / len(split))
        return jnp.repeat(jnp.exp(draws), shape[dim] // shards_of).reshape((-1,) + (1,) * (len(shape) - dim - 1))

    loudness = one(*split[0])
    for cut in split[1:]:
        loudness = loudness * one(*cut)
    return loudness


def bell_draw(own_key, shape, spread, limit, shards=(), kind=jnp.bfloat16):
    drawn = jax.random.normal(own_key, shape, jnp.float32) * spread
    if len(shards) > 0:
        drawn = shard_levels(own_key, shape, shards, -0.22, 0.18) * drawn
    return jnp.clip(drawn, min=-limit, max=limit).astype(kind)


def setup_inputs(seed: int = 0) -> dict:
    streams_of = jax.random.split(jax.random.key(seed), 7)
    noisy_image = bell_draw(streams_of[0], (NZ, NY, NX), 1.0, 6.0, ((0, 4), (1, 2), (2, 4)), jnp.float32)
    fidelity = jnp.clip(jnp.exp(math.log(8.0) - 2.7725887 * jax.random.uniform(streams_of[1], (NZ, NY, NX), jnp.float32) ** shard_levels(streams_of[1], (NZ, NY, NX), ((0, 4), (1, 2), (2, 4)), -0.2, 0.2)), 0.5, 8.0)
    primal_u = bell_draw(streams_of[2], (NZ, NY, NX), 1.0, 6.0, ((0, 4), (1, 2), (2, 4)), jnp.float32)
    primal_v = bell_draw(streams_of[3], (3, NZ, NY, NX), 0.3, 2.0, ((1, 4), (2, 2), (3, 4)), jnp.float32)
    dual_p = bell_draw(streams_of[4], (3, NZ, NY, NX), 0.4, 2.5, ((1, 4), (2, 2), (3, 4)), jnp.float32)
    dual_q = bell_draw(streams_of[5], (6, NZ, NY, NX), 0.4, 2.5, ((1, 4), (2, 2), (3, 4)), jnp.float32)
    return {"noisy_image": noisy_image, "fidelity": fidelity, "primal_u": primal_u, "primal_v": primal_v, "dual_p": dual_p, "dual_q": dual_q}


first_alpha = 0.5
second_alpha = 1.0
dual_step = 0.2
primal_step = 0.2
index_pairs = ((0, 0), (1, 1), (2, 2), (0, 1), (0, 2), (1, 2))

def pair_index(left_axis, right_axis):
    for position, entry_pair in enumerate(index_pairs):
        if entry_pair == (left_axis, right_axis) or entry_pair == (right_axis, left_axis):
            return position
    return 0

def shift_next(values, axis_dim):
    extent = values.shape[axis_dim]
    tail_part = lax.slice_in_dim(values, 1, extent, axis=axis_dim)
    zeros_shape = list(values.shape)
    zeros_shape[axis_dim] = 1
    return jnp.concatenate([tail_part, jnp.zeros(zeros_shape, values.dtype)], axis=axis_dim)

def shift_prev(values, axis_dim):
    extent = values.shape[axis_dim]
    head_part = lax.slice_in_dim(values, 0, extent - 1, axis=axis_dim)
    zeros_shape = list(values.shape)
    zeros_shape[axis_dim] = 1
    return jnp.concatenate([jnp.zeros(zeros_shape, values.dtype), head_part], axis=axis_dim)

def edge_masks(extents):
    lower_masks = []
    upper_masks = []
    for component in range(3):
        extent = extents[2 - component]
        places = lax.iota(jnp.int32, extent)
        shape_list = [1, 1, 1, 1]
        shape_list[3 - component] = extent
        upper_masks.append((places < extent - 1).astype(jnp.float32).reshape(shape_list))
        lower_masks.append((places > 0).astype(jnp.float32).reshape(shape_list))
    return (lower_masks, upper_masks)

def q_rows(stacked, column):
    return jnp.stack([stacked[pair_index(row_axis, column)] for row_axis in range(3)], axis=0)

def project(stacked, weights, bound):
    magnitude = jnp.sqrt(lax.optimization_barrier(jnp.sum(weights * stacked * stacked, axis=0, keepdims=True)))
    return stacked / jnp.maximum(1.0, magnitude / bound)

def dual_update(bar_u, bar_v, grad_dual, sym_dual, next_u, prev_v, lower_masks, upper_masks):
    grads = jnp.concatenate([upper_masks[component] * (next_u[component] - bar_u) for component in range(3)], axis=0)
    trial_p = grad_dual + dual_step * (grads - bar_v)
    new_p = project(trial_p, jnp.ones((3, 1, 1, 1), jnp.float32), first_alpha)
    derivs = [lower_masks[component] * (bar_v - prev_v[component]) for component in range(3)]
    sym_parts = []
    for left_axis, right_axis in index_pairs:
        sym_parts.append(0.5 * (derivs[right_axis][left_axis] + derivs[left_axis][right_axis]))
    trial_q = sym_dual + dual_step * jnp.stack(sym_parts, axis=0)
    weights = jnp.array([1.0, 1.0, 1.0, 2.0, 2.0, 2.0], jnp.float32).reshape((6, 1, 1, 1))
    new_q = project(trial_q, weights, second_alpha)
    return (new_p, new_q)

def primal_update(image_u, vector_v, grad_dual, sym_dual, noisy, weight_map, prev_p, next_q, lower_masks, upper_masks):
    divergence = jnp.zeros_like(image_u)
    second_div = jnp.zeros_like(vector_v)
    for component in range(3):
        divergence = divergence + upper_masks[component] * grad_dual[component:component + 1] - prev_p[component]
        second_div = second_div + next_q[component] - lower_masks[component] * q_rows(sym_dual, component)
    new_u = (image_u + primal_step * divergence + primal_step * weight_map * noisy) / (1.0 + primal_step * weight_map)
    new_v = vector_v + primal_step * (grad_dual + second_div)
    return (new_u, new_v)

def reference(noisy_image, fidelity, primal_u, primal_v, dual_p, dual_q):
    noisy = noisy_image[None]
    weight_map = fidelity[None]
    image_u = primal_u[None]
    vector_v = primal_v
    grad_dual = dual_p
    sym_dual = dual_q
    lower_masks, upper_masks = edge_masks(noisy_image.shape)
    bar_u = image_u
    bar_v = vector_v
    for step_index in range(ITERS):
        next_u = [shift_next(bar_u, 3 - component) for component in range(3)]
        prev_v = [shift_prev(bar_v, 3 - component) for component in range(3)]
        grad_dual, sym_dual = dual_update(bar_u, bar_v, grad_dual, sym_dual, next_u, prev_v, lower_masks, upper_masks)
        prev_p = [shift_prev(grad_dual[component:component + 1], 3 - component) for component in range(3)]
        next_q = [shift_next(q_rows(sym_dual, component), 3 - component) for component in range(3)]
        new_u, new_v = primal_update(image_u, vector_v, grad_dual, sym_dual, noisy, weight_map, prev_p, next_q, lower_masks, upper_masks)
        bar_u = 2.0 * new_u - image_u
        bar_v = 2.0 * new_v - vector_v
        image_u = new_u
        vector_v = new_v
    return (image_u[0], vector_v, grad_dual, sym_dual)
```

```python
import functools

import jax
import jax.numpy as jnp
from jax import lax
from jax.experimental import pallas as pl
from jax.experimental.pallas import tpu as pltpu
from jax.sharding import PartitionSpec as P

ITERS = 3
AXES = ("gx", "gy", "gz")
ALPHA1, ALPHA0, SIGMA, TAU = 0.5, 1.0, 0.2, 0.2
Q_FROM = (0, 3, 1, 5, 2, 4)
XX, XY, YY, YZ, ZZ, XZ = range(6)
MESH = pl.DeviceIdType.MESH
TOP = 8


def kernel(
    noisy_in, fid_in, u_in, v_in, p_in, q_in,
    u_out, v_out, p_out, q_out,
    bar, pp, qq, gain, offset,
    send_u, send_v, send_p, send_q, got_u, got_v, got_p, got_q,
    load_sem, send_sem, recv_sem,
):
    zs, ys, xs = u_in.shape
    blocks = ys // 8
    place = [lax.axis_index(a) for a in AXES]
    count = [lax.axis_size(a) for a in AXES]
    below = [place[i] > 0 for i in range(3)]
    above = [place[i] < count[i] - 1 for i in range(3)]

    peers = sum(there.astype(jnp.int32) for there in below + above)

    barrier = pltpu.get_barrier_semaphore()
    for i in range(3):
        for there, by in ((below[i], -1), (above[i], 1)):
            @pl.when(there)
            def _():
                pl.semaphore_signal(
                    barrier, inc=1, device_id={AXES[i]: place[i] + by}, device_id_type=MESH
                )

    mid_z, mid_y = pl.ds(1, zs), pl.ds(TOP, ys)
    loads = [
        pltpu.make_async_copy(u_in, bar.at[0, mid_z, mid_y], load_sem.at[0]),
        pltpu.make_async_copy(v_in, bar.at[pl.ds(1, 3), mid_z, mid_y], load_sem.at[1]),
        pltpu.make_async_copy(p_in, pp.at[:, mid_z, mid_y], load_sem.at[2]),
        pltpu.make_async_copy(noisy_in, offset, load_sem.at[3]),
        pltpu.make_async_copy(fid_in, gain, load_sem.at[4]),
    ] + [
        pltpu.make_async_copy(q_in.at[Q_FROM[k]], qq.at[k, mid_z, mid_y], load_sem.at[5 + k])
        for k in range(6)
    ]
    for load in loads:
        load.start()

    row = jnp.zeros((zs + 2, 1, xs), jnp.float32)
    layer = jnp.zeros((ys, xs), jnp.float32)

    @pl.when(jnp.logical_not(below[0]))
    def _():
        got_v[...] = layer
        got_p[...] = layer

    @pl.when(jnp.logical_not(above[0]))
    def _():
        got_u[...] = layer
        got_q[...] = layer

    @pl.when(jnp.logical_not(below[1]))
    def _():
        for k in range(3):
            bar[1 + k, :, TOP - 1 : TOP, :] = row
        pp[1, :, TOP - 1 : TOP, :] = row

    @pl.when(jnp.logical_not(above[1]))
    def _():
        bar[0, :, TOP + ys : TOP + ys + 1, :] = row
        for k in (XY, YY, YZ):
            qq[k, :, TOP + ys : TOP + ys + 1, :] = row

    @pl.when(jnp.logical_not(below[2]))
    def _():
        for k in range(3):
            bar[1 + k, 0, TOP : TOP + ys, :] = layer
        pp[2, 0, TOP : TOP + ys, :] = layer

    @pl.when(jnp.logical_not(above[2]))
    def _():
        bar[0, zs + 1, TOP : TOP + ys, :] = layer
        for k in (YZ, ZZ, XZ):
            qq[k, zs + 1, TOP : TOP + ys, :] = layer

    lane = lax.broadcasted_iota(jnp.int32, (8, xs), 1)
    sub = lax.broadcasted_iota(jnp.int32, (8, xs), 0)
    first_lane, last_lane = lane == 0, lane == xs - 1

    def factor(flag):
        return jnp.where(flag, jnp.float32(1), jnp.float32(0))

    up_x = jnp.where(last_lane, factor(above[0]), 1.0)
    lo_x = jnp.where(first_lane, factor(below[0]), 1.0)
    up_y_last = jnp.where(sub == 7, factor(above[1]), 1.0)
    lo_y_first = jnp.where(sub == 0, factor(below[1]), 1.0)

    def up_z(z):
        return jnp.where(jnp.logical_or(z < zs - 1, above[2]), jnp.float32(1), jnp.float32(0))

    def lo_z(z):
        return jnp.where(jnp.logical_or(z > 0, below[2]), jnp.float32(1), jnp.float32(0))

    def up_y(b, value):
        return up_y_last * value if b == blocks - 1 else value

    def lo_y(b, value):
        return lo_y_first * value if b == 0 else value

    def next_x(value, got, k, z):
        return jnp.where(
            last_lane, pltpu.roll(got, xs - 1 - k * zs - z, 1), pltpu.roll(value, xs - 1, 1)
        )

    def prev_x(value, got, k, z):
        return jnp.where(
            first_lane, pltpu.roll(got, xs - 1 - k * zs - z, 1), pltpu.roll(value, 1, 1)
        )

    def pack_first(packed, value, k, z):
        return jnp.where(lane == k * zs + z, pltpu.roll(value, k * zs + z, 1), packed)

    def pack_last(packed, value, k, z):
        return jnp.where(lane == k * zs + z + 1, pltpu.roll(value, k * zs + z + 2, 1), packed)

    def down(src, dst, i, k):
        return (
            pltpu.make_async_remote_copy(
                src_ref=src, dst_ref=dst, send_sem=send_sem.at[k], recv_sem=recv_sem.at[k],
                device_id={AXES[i]: place[i] - 1}, device_id_type=MESH,
            ),
            below[i],
            above[i],
        )

    def up(src, dst, i, k):
        return (
            pltpu.make_async_remote_copy(
                src_ref=src, dst_ref=dst, send_sem=send_sem.at[k], recv_sem=recv_sem.at[k],
                device_id={AXES[i]: place[i] + 1}, device_id_type=MESH,
            ),
            above[i],
            below[i],
        )

    comps = pl.ds(1, 3)
    primal_moves = [
        up(bar.at[comps, zs, mid_y], bar.at[comps, 0, mid_y], 2, 0),
        down(bar.at[0, 1, mid_y], bar.at[0, zs + 1, mid_y], 2, 1),
        up(bar.at[comps, mid_z, TOP + ys - 1], bar.at[comps, mid_z, TOP - 1], 1, 2),
        down(bar.at[0, mid_z, TOP], bar.at[0, mid_z, TOP + ys], 1, 3),
        up(send_v, got_v, 0, 4),
        down(send_u, got_u, 0, 5),
    ]
    dual_moves = [
        down(qq.at[pl.ds(YZ, 3), 1, mid_y], qq.at[pl.ds(YZ, 3), zs + 1, mid_y], 2, 6),
        up(pp.at[2, zs, mid_y], pp.at[2, 0, mid_y], 2, 7),
        down(qq.at[pl.ds(XY, 3), mid_z, TOP], qq.at[pl.ds(XY, 3), mid_z, TOP + ys], 1, 8),
        up(pp.at[1, mid_z, TOP + ys - 1], pp.at[1, mid_z, TOP - 1], 1, 9),
        down(send_q, got_q, 0, 10),
        up(send_p, got_p, 0, 11),
    ]

    def start(moves):
        for copy, goes, comes in moves:
            @pl.when(goes)
            def _():
                copy.start()

    def finish(moves):
        for copy, goes, comes in moves:
            @pl.when(goes)
            def _():
                copy.wait_send()

            @pl.when(comes)
            def _():
                copy.wait_recv()

    empty = jnp.zeros((8, xs), jnp.float32)

    def rows(b, by=0):
        return pl.ds(TOP + 8 * b + by, 8)

    def store_packed(ref, packed):
        for b in range(blocks):
            ref[pl.ds(8 * b, 8), :] = packed[b]

    for load in loads[:2]:
        load.wait()

    def first_faces(z, packed):
        first, last = list(packed[0]), list(packed[1])
        for b in range(blocks):
            first[b] = pack_first(first[b], bar[0, z + 1, rows(b), :], 0, z)
            for k in range(3):
                last[b] = pack_last(last[b], bar[1 + k, z + 1, rows(b), :], k, z)
        return tuple(first), tuple(last)

    nothing = (empty,) * blocks
    first, last = lax.fori_loop(0, zs, first_faces, (nothing, nothing))
    store_packed(send_u, first)
    store_packed(send_v, last)
    pl.semaphore_wait(barrier, peers)
    start(primal_moves)

    for load in loads[2:]:
        load.wait()

    def prepare(z, carry):
        weight = TAU * gain[z]
        inverse = 1.0 / (1.0 + weight)
        gain[z] = inverse
        offset[z] = weight * offset[z] * inverse
        return carry

    lax.fori_loop(0, zs, prepare, 0)

    for step in range(ITERS):
        last_step = step == ITERS - 1
        finish(primal_moves)

        def dual(z, packed):
            of_p, of_q = list(packed[0]), list(packed[1])
            z_up, z_lo = SIGMA * up_z(z), (0.5 * SIGMA) * lo_z(z)
            for b in range(blocks):
                r, here = rows(b), pl.ds(8 * b, 8)
                u = bar[0, z + 1, r, :]
                v = [bar[1 + k, z + 1, r, :] for k in range(3)]
                t = [
                    pp[0, z + 1, r, :] + SIGMA * (up_x * (next_x(u, got_u[here, :], 0, z) - u) - v[0]),
                    pp[1, z + 1, r, :]
                    + SIGMA * (up_y(b, bar[0, z + 1, rows(b, 1), :] - u) - v[1]),
                    pp[2, z + 1, r, :] + (z_up * (bar[0, z + 2, r, :] - u) - SIGMA * v[2]),
                ]
                size = t[0] * t[0] + t[1] * t[1] + t[2] * t[2]
                scale = jnp.minimum(1.0, ALPHA1 * lax.rsqrt(size))
                t = [scale * part for part in t]
                for k in range(3):
                    pp[k, z + 1, r, :] = t[k]
                    if last_step:
                        p_out[k, z, here, :] = t[k]
                of_p[b] = pack_last(of_p[b], t[0], 0, z)

                half_lo_x = (0.5 * SIGMA) * lo_x
                received = got_v[here, :]
                dx = [half_lo_x * (v[k] - prev_x(v[k], received, k, z)) for k in range(3)]
                dy = [
                    lo_y(b, (0.5 * SIGMA) * (v[k] - bar[1 + k, z + 1, rows(b, -1), :]))
                    for k in range(3)
                ]
                dz = [z_lo * (v[k] - bar[1 + k, z, r, :]) for k in range(3)]
                s = [None] * 6
                s[XX] = qq[XX, z + 1, r, :] + 2.0 * dx[0]
                s[YY] = qq[YY, z + 1, r, :] + 2.0 * dy[1]
                s[ZZ] = qq[ZZ, z + 1, r, :] + 2.0 * dz[2]
                s[XY] = qq[XY, z + 1, r, :] + (dy[0] + dx[1])
                s[XZ] = qq[XZ, z + 1, r, :] + (dz[0] + dx[2])
                s[YZ] = qq[YZ, z + 1, r, :] + (dz[1] + dy[2])
                size = (s[XX] * s[XX] + s[YY] * s[YY] + s[ZZ] * s[ZZ]) + 2.0 * (
                    s[XY] * s[XY] + s[XZ] * s[XZ] + s[YZ] * s[YZ]
                )
                scale = jnp.minimum(1.0, ALPHA0 * lax.rsqrt(size))
                s = [scale * part for part in s]
                for k in range(6):
                    qq[k, z + 1, r, :] = s[k]
                    if last_step:
                        q_out[Q_FROM[k], z, here, :] = s[k]
                for k, part in enumerate((XX, XY, XZ)):
                    of_q[b] = pack_first(of_q[b], s[part], k, z)
            return tuple(of_p), tuple(of_q)

        of_p, of_q = lax.fori_loop(0, zs, dual, (nothing, nothing))
        store_packed(send_p, of_p)
        store_packed(send_q, of_q)
        start(dual_moves)
        finish(dual_moves)

        def primal(z, packed):
            of_u, of_v = list(packed[0]), list(packed[1])
            z_up, z_lo = up_z(z), lo_z(z)
            for b in range(blocks):
                r, here = rows(b), pl.ds(8 * b, 8)
                p = [pp[k, z + 1, r, :] for k in range(3)]
                div = (
                    (up_x * p[0] - prev_x(p[0], got_p[here, :], 0, z))
                    + (up_y(b, p[1]) - pp[1, z + 1, rows(b, -1), :])
                    + (z_up * p[2] - pp[2, z, r, :])
                )
                q = [qq[k, z + 1, r, :] for k in range(6)]
                received = got_q[here, :]
                new_v = []
                for k, (ax, ay, az) in enumerate(((XX, XY, XZ), (XY, YY, YZ), (XZ, YZ, ZZ))):
                    div2 = (
                        (next_x(q[ax], received, k, z) - lo_x * q[ax])
                        + (qq[ay, z + 1, rows(b, 1), :] - lo_y(b, q[ay]))
                        + (qq[az, z + 2, r, :] - z_lo * q[az])
                    )
                    old = bar[1 + k, z + 1, r, :] if step == 0 else v_out[k, z, here, :]
                    new = old + TAU * (p[k] + div2)
                    v_out[k, z, here, :] = new
                    if not last_step:
                        ahead = 2.0 * new - old
                        bar[1 + k, z + 1, r, :] = ahead
                        of_v[b] = pack_last(of_v[b], ahead, k, z)
                old = bar[0, z + 1, r, :] if step == 0 else u_out[z, here, :]
                new = (old + TAU * div) * gain[z, here, :] + offset[z, here, :]
                u_out[z, here, :] = new
                if not last_step:
                    ahead = 2.0 * new - old
                    bar[0, z + 1, r, :] = ahead
                    of_u[b] = pack_first(of_u[b], ahead, 0, z)
            return tuple(of_u), tuple(of_v)

        of_u, of_v = lax.fori_loop(0, zs, primal, (nothing, nothing))
        if not last_step:
            store_packed(send_u, of_u)
            store_packed(send_v, of_v)
            start(primal_moves)


def per_device(noisy_image, fidelity, primal_u, primal_v, dual_p, dual_q):
    zs, ys, xs = primal_u.shape
    assert xs == 128 and ys % 8 == 0 and 3 * zs < xs
    f32 = jnp.float32
    padded = (zs + 2, ys + 2 * TOP, xs)
    face = pltpu.VMEM((ys, xs), f32)
    return pl.pallas_call(
        kernel,
        out_shape=tuple(pltpu.VMEM(a.shape, f32) for a in (primal_u, primal_v, dual_p, dual_q)),
        in_specs=[pl.BlockSpec(memory_space=pl.ANY)] * 6,
        out_specs=tuple([pl.BlockSpec(memory_space=pltpu.VMEM)] * 4),
        scratch_shapes=[
            pltpu.VMEM((4,) + padded, f32),
            pltpu.VMEM((3,) + padded, f32),
            pltpu.VMEM((6,) + padded, f32),
            pltpu.VMEM((zs, ys, xs), f32),
            pltpu.VMEM((zs, ys, xs), f32),
        ]
        + [face] * 8
        + [
            pltpu.SemaphoreType.DMA((11,)),
            pltpu.SemaphoreType.DMA((12,)),
            pltpu.SemaphoreType.DMA((12,)),
        ],
        compiler_params=pltpu.CompilerParams(collective_id=0, has_side_effects=True),
        name="tgv",
    )(noisy_image, fidelity, primal_u, primal_v, dual_p, dual_q)


def solution(mesh):
    scalar, stack = P("gz", "gy", "gx"), P(None, "gz", "gy", "gx")
    return jax.shard_map(
        per_device,
        mesh=mesh,
        in_specs=(scalar, scalar, scalar, stack, stack, stack),
        out_specs=(scalar, stack, stack, stack),
        check_vma=False,
    )
```

```python
import functools

import jax
import jax.numpy as jnp
from jax import lax
from jax.experimental import pallas as pl
from jax.experimental.pallas import tpu as pltpu
from jax.sharding import PartitionSpec as P

ITERS = 3
AXES = ("gx", "gy", "gz")
ALPHA1, ALPHA0, SIGMA, TAU = 0.5, 1.0, 0.2, 0.2
Q_FROM = (0, 3, 1, 5, 2, 4)
GROUP = 4
XX, XY, YY, YZ, ZZ, XZ = range(6)
MESH = pl.DeviceIdType.MESH
TOP = 8


def kernel(
    noisy_in, fid_in, u_in, v_in, p_in, q_in,
    u_out, v_out, p_out, q_out,
    bar, pp, qq, gain, offset,
    send_u, send_v, send_p, send_q, got_u, got_v, got_p, got_q,
    load_sem, send_sem, recv_sem,
):
    zs, ys, xs = u_in.shape
    blocks = ys // 8
    place = [lax.axis_index(a) for a in AXES]
    count = [lax.axis_size(a) for a in AXES]
    below = [place[i] > 0 for i in range(3)]
    above = [place[i] < count[i] - 1 for i in range(3)]

    peers = sum(there.astype(jnp.int32) for there in below + above)

    barrier = pltpu.get_barrier_semaphore()
    for i in range(3):
        for there, by in ((below[i], -1), (above[i], 1)):
            @pl.when(there)
            def _():
                pl.semaphore_signal(
                    barrier, inc=1, device_id={AXES[i]: place[i] + by}, device_id_type=MESH
                )

    mid_z, mid_y = pl.ds(1, zs), pl.ds(TOP, ys)
    loads = [
        pltpu.make_async_copy(u_in, bar.at[0, mid_z, mid_y], load_sem.at[0]),
        pltpu.make_async_copy(v_in, bar.at[pl.ds(1, 3), mid_z, mid_y], load_sem.at[1]),
        pltpu.make_async_copy(p_in, pp.at[:, mid_z, mid_y], load_sem.at[2]),
        pltpu.make_async_copy(noisy_in, offset, load_sem.at[3]),
        pltpu.make_async_copy(fid_in, gain, load_sem.at[4]),
    ] + [
        pltpu.make_async_copy(q_in.at[Q_FROM[k]], qq.at[k, mid_z, mid_y], load_sem.at[5 + k])
        for k in range(6)
    ]
    for load in loads:
        load.start()

    row = jnp.zeros((zs + 2, 1, xs), jnp.float32)
    layer = jnp.zeros((ys, xs), jnp.float32)

    @pl.when(jnp.logical_not(below[0]))
    def _():
        got_v[...] = layer
        got_p[...] = layer

    @pl.when(jnp.logical_not(above[0]))
    def _():
        got_u[...] = layer
        got_q[...] = layer

    @pl.when(jnp.logical_not(below[1]))
    def _():
        for k in range(3):
            bar[1 + k, :, TOP - 1 : TOP, :] = row
        pp[1, :, TOP - 1 : TOP, :] = row

    @pl.when(jnp.logical_not(above[1]))
    def _():
        bar[0, :, TOP + ys : TOP + ys + 1, :] = row
        for k in (XY, YY, YZ):
            qq[k, :, TOP + ys : TOP + ys + 1, :] = row

    @pl.when(jnp.logical_not(below[2]))
    def _():
        for k in range(3):
            bar[1 + k, 0, TOP : TOP + ys, :] = layer
        pp[2, 0, TOP : TOP + ys, :] = layer

    @pl.when(jnp.logical_not(above[2]))
    def _():
        bar[0, zs + 1, TOP : TOP + ys, :] = layer
        for k in (YZ, ZZ, XZ):
            qq[k, zs + 1, TOP : TOP + ys, :] = layer

    lane = lax.broadcasted_iota(jnp.int32, (8, xs), 1)
    sub = lax.broadcasted_iota(jnp.int32, (8, xs), 0)
    first_lane, last_lane = lane == 0, lane == xs - 1

    def factor(flag):
        return jnp.where(flag, jnp.float32(1), jnp.float32(0))

    up_x = jnp.where(last_lane, factor(above[0]), 1.0)
    lo_x = jnp.where(first_lane, factor(below[0]), 1.0)
    up_y_last = jnp.where(sub == 7, factor(above[1]), 1.0)
    lo_y_first = jnp.where(sub == 0, factor(below[1]), 1.0)

    def flush(later):
        for ref, at, value in later:
            ref[at + (slice(None),)] = value
        later.clear()

    def sweep(body, moves, wanted):
        def turn(j, packed):
            one, two = list(packed[0]), list(packed[1])
            body(jnp.where(j == 0, 0, 2 * j - 1), one, two)
            body(jnp.where(j == 0, zs - 1, 2 * j), one, two)

            @pl.when(jnp.logical_and(wanted, j == 0))
            def _():
                start(moves)

            return tuple(one), tuple(two)

        return lax.fori_loop(0, zs // 2, turn, (nothing, nothing))

    def up_z(z):
        return factor(jnp.logical_or(z < zs - 1, above[2]))

    def lo_z(z):
        return factor(jnp.logical_or(z > 0, below[2]))

    def up_y(b, value):
        return up_y_last * value if b == blocks - 1 else value

    def lo_y(b, value):
        return lo_y_first * value if b == 0 else value

    def next_x(value, got, k, z):
        return jnp.where(
            last_lane, pltpu.roll(got, xs - 1 - k * zs - z, 1), pltpu.roll(value, xs - 1, 1)
        )

    def prev_x(value, got, k, z):
        return jnp.where(
            first_lane, pltpu.roll(got, xs - 1 - k * zs - z, 1), pltpu.roll(value, 1, 1)
        )

    def pack_first(packed, value, k, z):
        return jnp.where(lane == k * zs + z, pltpu.roll(value, k * zs + z, 1), packed)

    def pack_last(packed, value, k, z):
        return jnp.where(lane == k * zs + z + 1, pltpu.roll(value, k * zs + z + 2, 1), packed)

    def down(src, dst, i, k):
        return (
            pltpu.make_async_remote_copy(
                src_ref=src, dst_ref=dst, send_sem=send_sem.at[k], recv_sem=recv_sem.at[k],
                device_id={AXES[i]: place[i] - 1}, device_id_type=MESH,
            ),
            below[i],
            above[i],
        )

    def up(src, dst, i, k):
        return (
            pltpu.make_async_remote_copy(
                src_ref=src, dst_ref=dst, send_sem=send_sem.at[k], recv_sem=recv_sem.at[k],
                device_id={AXES[i]: place[i] + 1}, device_id_type=MESH,
            ),
            above[i],
            below[i],
        )

    comps = pl.ds(1, 3)
    primal_moves = [
        up(bar.at[comps, zs, mid_y], bar.at[comps, 0, mid_y], 2, 0),
        down(bar.at[0, 1, mid_y], bar.at[0, zs + 1, mid_y], 2, 1),
        up(bar.at[comps, mid_z, TOP + ys - 1], bar.at[comps, mid_z, TOP - 1], 1, 2),
        down(bar.at[0, mid_z, TOP], bar.at[0, mid_z, TOP + ys], 1, 3),
        up(send_v, got_v, 0, 4),
        down(send_u, got_u, 0, 5),
    ]
    dual_moves = [
        down(qq.at[pl.ds(YZ, 3), 1, mid_y], qq.at[pl.ds(YZ, 3), zs + 1, mid_y], 2, 6),
        up(pp.at[2, zs, mid_y], pp.at[2, 0, mid_y], 2, 7),
        down(qq.at[pl.ds(XY, 3), mid_z, TOP], qq.at[pl.ds(XY, 3), mid_z, TOP + ys], 1, 8),
        up(pp.at[1, mid_z, TOP + ys - 1], pp.at[1, mid_z, TOP - 1], 1, 9),
        down(send_q, got_q, 0, 10),
        up(send_p, got_p, 0, 11),
    ]

    def start(moves):
        for copy, goes, comes in moves:
            @pl.when(goes)
            def _():
                copy.start()

    def finish(moves):
        for copy, goes, comes in moves:
            @pl.when(goes)
            def _():
                copy.wait_send()

            @pl.when(comes)
            def _():
                copy.wait_recv()

    empty = jnp.zeros((8, xs), jnp.float32)

    def rows(b, by=0):
        return pl.ds(TOP + 8 * b + by, 8)

    def store_packed(ref, packed):
        for b in range(blocks):
            ref[pl.ds(8 * b, 8), :] = packed[b]

    for load in loads[:2]:
        load.wait()

    def first_faces(z, packed):
        first, last = list(packed[0]), list(packed[1])
        for b in range(blocks):
            first[b] = pack_first(first[b], bar[0, z + 1, rows(b), :], 0, z)
            for k in range(3):
                last[b] = pack_last(last[b], bar[1 + k, z + 1, rows(b), :], k, z)
        return tuple(first), tuple(last)

    nothing = (empty,) * blocks
    first, last = lax.fori_loop(0, zs, first_faces, (nothing, nothing))
    store_packed(send_u, first)
    store_packed(send_v, last)
    pl.semaphore_wait(barrier, peers)
    start(primal_moves)

    for load in loads[2:]:
        load.wait()

    def prepare(z, carry):
        weight = TAU * gain[z]
        inverse = 1.0 / (1.0 + weight)
        gain[z] = inverse
        offset[z] = weight * offset[z] * inverse
        u_out[z] = bar[0, z + 1, mid_y, :]
        for k in range(3):
            v_out[k, z] = bar[1 + k, z + 1, mid_y, :]
        return carry

    lax.fori_loop(0, zs, prepare, 0)

    def iteration(step, carry):
        more = step < ITERS - 1
        finish(primal_moves)

        def dual(z, of_p, of_q):
            z_up, z_lo = SIGMA * up_z(z), (0.5 * SIGMA) * lo_z(z)
            later = []
            for b in range(blocks):
                if b % GROUP == 0:
                    flush(later)
                r, here = rows(b), pl.ds(8 * b, 8)
                u = bar[0, z + 1, r, :]
                v = [bar[1 + k, z + 1, r, :] for k in range(3)]
                t = [
                    pp[0, z + 1, r, :] + SIGMA * (up_x * (next_x(u, got_u[here, :], 0, z) - u) - v[0]),
                    pp[1, z + 1, r, :]
                    + SIGMA * (up_y(b, bar[0, z + 1, rows(b, 1), :] - u) - v[1]),
                    pp[2, z + 1, r, :] + (z_up * (bar[0, z + 2, r, :] - u) - SIGMA * v[2]),
                ]
                size = t[0] * t[0] + t[1] * t[1] + t[2] * t[2]
                scale = jnp.minimum(1.0, ALPHA1 * lax.rsqrt(size))
                t = [scale * part for part in t]
                for k in range(3):
                    later.append((pp, (k, z + 1, r), t[k]))
                    later.append((p_out, (k, z, here), t[k]))
                of_p[b] = pack_last(of_p[b], t[0], 0, z)

                half_lo_x = (0.5 * SIGMA) * lo_x
                received = got_v[here, :]
                dx = [half_lo_x * (v[k] - prev_x(v[k], received, k, z)) for k in range(3)]
                dy = [
                    lo_y(b, (0.5 * SIGMA) * (v[k] - bar[1 + k, z + 1, rows(b, -1), :]))
                    for k in range(3)
                ]
                dz = [z_lo * (v[k] - bar[1 + k, z, r, :]) for k in range(3)]
                s = [None] * 6
                s[XX] = qq[XX, z + 1, r, :] + 2.0 * dx[0]
                s[YY] = qq[YY, z + 1, r, :] + 2.0 * dy[1]
                s[ZZ] = qq[ZZ, z + 1, r, :] + 2.0 * dz[2]
                s[XY] = qq[XY, z + 1, r, :] + (dy[0] + dx[1])
                s[XZ] = qq[XZ, z + 1, r, :] + (dz[0] + dx[2])
                s[YZ] = qq[YZ, z + 1, r, :] + (dz[1] + dy[2])
                size = (s[XX] * s[XX] + s[YY] * s[YY] + s[ZZ] * s[ZZ]) + 2.0 * (
                    s[XY] * s[XY] + s[XZ] * s[XZ] + s[YZ] * s[YZ]
                )
                scale = jnp.minimum(1.0, ALPHA0 * lax.rsqrt(size))
                s = [scale * part for part in s]
                for k in range(6):
                    later.append((qq, (k, z + 1, r), s[k]))
                    later.append((q_out, (Q_FROM[k], z, here), s[k]))
                for k, part in enumerate((XX, XY, XZ)):
                    of_q[b] = pack_first(of_q[b], s[part], k, z)
            flush(later)

        of_p, of_q = sweep(dual, dual_moves[:2], True)
        store_packed(send_p, of_p)
        store_packed(send_q, of_q)
        start(dual_moves[2:])
        finish(dual_moves)

        def primal(z, of_u, of_v):
            z_up, z_lo = up_z(z), lo_z(z)
            later = []
            for b in range(blocks):
                if b % GROUP == 0:
                    flush(later)
                r, here = rows(b), pl.ds(8 * b, 8)
                p = [pp[k, z + 1, r, :] for k in range(3)]
                div = (
                    (up_x * p[0] - prev_x(p[0], got_p[here, :], 0, z))
                    + (up_y(b, p[1]) - pp[1, z + 1, rows(b, -1), :])
                    + (z_up * p[2] - pp[2, z, r, :])
                )
                q = [qq[k, z + 1, r, :] for k in range(6)]
                received = got_q[here, :]
                new_v = []
                for k, (ax, ay, az) in enumerate(((XX, XY, XZ), (XY, YY, YZ), (XZ, YZ, ZZ))):
                    div2 = (
                        (next_x(q[ax], received, k, z) - lo_x * q[ax])
                        + (qq[ay, z + 1, rows(b, 1), :] - lo_y(b, q[ay]))
                        + (qq[az, z + 2, r, :] - z_lo * q[az])
                    )
                    old = v_out[k, z, here, :]
                    new = old + TAU * (p[k] + div2)
                    later.append((v_out, (k, z, here), new))
                    ahead = 2.0 * new - old
                    later.append((bar, (1 + k, z + 1, r), ahead))
                    of_v[b] = pack_last(of_v[b], ahead, k, z)
                old = u_out[z, here, :]
                new = (old + TAU * div) * gain[z, here, :] + offset[z, here, :]
                later.append((u_out, (z, here), new))
                ahead = 2.0 * new - old
                later.append((bar, (0, z + 1, r), ahead))
                of_u[b] = pack_first(of_u[b], ahead, 0, z)
            flush(later)

        of_u, of_v = sweep(primal, primal_moves[:2], more)

        @pl.when(more)
        def _():
            store_packed(send_u, of_u)
            store_packed(send_v, of_v)
            start(primal_moves[2:])

        return carry

    lax.fori_loop(0, ITERS, iteration, 0)


def copy_out(u_in, v_in, p_in, q_in, u_out, v_out, p_out, q_out, sems):
    pairs = ((q_in, q_out), (p_in, p_out), (v_in, v_out), (u_in, u_out))
    copies = [pltpu.make_async_copy(a, b, sems.at[i]) for i, (a, b) in enumerate(pairs)]
    for copy in copies:
        copy.start()
    for copy in copies:
        copy.wait()


def per_device(noisy_image, fidelity, primal_u, primal_v, dual_p, dual_q):
    zs, ys, xs = primal_u.shape
    assert xs == 128 and ys % 8 == 0 and zs % 2 == 0 and 3 * zs < xs
    f32 = jnp.float32
    padded = (zs + 2, ys + 2 * TOP, xs)
    face = pltpu.VMEM((ys, xs), f32)
    results = pl.pallas_call(
        kernel,
        out_shape=tuple(pltpu.VMEM(a.shape, f32) for a in (primal_u, primal_v, dual_p, dual_q)),
        in_specs=[pl.BlockSpec(memory_space=pl.ANY)] * 6,
        out_specs=tuple([pl.BlockSpec(memory_space=pltpu.VMEM)] * 4),
        scratch_shapes=[
            pltpu.VMEM((4,) + padded, f32),
            pltpu.VMEM((3,) + padded, f32),
            pltpu.VMEM((6,) + padded, f32),
            pltpu.VMEM((zs, ys, xs), f32),
            pltpu.VMEM((zs, ys, xs), f32),
        ]
        + [face] * 8
        + [
            pltpu.SemaphoreType.DMA((11,)),
            pltpu.SemaphoreType.DMA((12,)),
            pltpu.SemaphoreType.DMA((12,)),
        ],
        compiler_params=pltpu.CompilerParams(collective_id=0, has_side_effects=True),
        name="tgv",
    )(noisy_image, fidelity, primal_u, primal_v, dual_p, dual_q)
    return pl.pallas_call(
        copy_out,
        out_shape=tuple(jax.ShapeDtypeStruct(a.shape, f32) for a in results),
        in_specs=[pl.BlockSpec(memory_space=pltpu.VMEM)] * 4,
        out_specs=tuple([pl.BlockSpec(memory_space=pl.ANY)] * 4),
        scratch_shapes=[pltpu.SemaphoreType.DMA((4,))],
        name="out",
    )(*[pltpu.with_memory_space_constraint(r, pltpu.VMEM) for r in results])


def solution(mesh):
    scalar, stack = P("gz", "gy", "gx"), P(None, "gz", "gy", "gx")
    return jax.shard_map(
        per_device,
        mesh=mesh,
        in_specs=(scalar, scalar, scalar, stack, stack, stack),
        out_specs=(scalar, stack, stack, stack),
        check_vma=False,
    )
```

```python
import functools

import jax
import jax.numpy as jnp
from jax import lax
from jax.experimental import pallas as pl
from jax.experimental.pallas import tpu as pltpu
from jax.sharding import PartitionSpec as P

ITERS = 3
AXES = ("gx", "gy", "gz")
ALPHA1, ALPHA0, SIGMA, TAU = 0.5, 1.0, 0.2, 0.2
Q_FROM = (0, 3, 1, 5, 2, 4)
GROUP = 4
XX, XY, YY, YZ, ZZ, XZ = range(6)
MESH = pl.DeviceIdType.MESH
TOP = 8


def kernel(
    noisy_in, fid_in, u_in, v_in, p_in, q_in,
    u_out, v_out, p_out, q_out,
    bar, pp, qq, gain, offset, partial,
    send_u, send_v, send_p, send_q, got_u, got_v, got_p, got_q,
    load_sem, send_sem, recv_sem,
):
    zs, ys, xs = u_in.shape
    blocks = ys // 8
    place = [lax.axis_index(a) for a in AXES]
    count = [lax.axis_size(a) for a in AXES]
    below = [place[i] > 0 for i in range(3)]
    above = [place[i] < count[i] - 1 for i in range(3)]

    peers = sum(there.astype(jnp.int32) for there in below + above)

    barrier = pltpu.get_barrier_semaphore()
    for i in range(3):
        for there, by in ((below[i], -1), (above[i], 1)):
            @pl.when(there)
            def _():
                pl.semaphore_signal(
                    barrier, inc=1, device_id={AXES[i]: place[i] + by}, device_id_type=MESH
                )

    mid_z, mid_y = pl.ds(1, zs), pl.ds(TOP, ys)
    loads = [
        pltpu.make_async_copy(u_in, bar.at[0, mid_z, mid_y], load_sem.at[0]),
        pltpu.make_async_copy(v_in, bar.at[pl.ds(1, 3), mid_z, mid_y], load_sem.at[1]),
        pltpu.make_async_copy(p_in, pp.at[:, mid_z, mid_y], load_sem.at[2]),
        pltpu.make_async_copy(noisy_in, offset, load_sem.at[3]),
        pltpu.make_async_copy(fid_in, gain, load_sem.at[4]),
    ] + [
        pltpu.make_async_copy(q_in.at[Q_FROM[k]], qq.at[k, mid_z, mid_y], load_sem.at[5 + k])
        for k in range(6)
    ]
    for load in loads:
        load.start()

    row = jnp.zeros((zs + 2, 1, xs), jnp.float32)
    layer = jnp.zeros((ys, xs), jnp.float32)

    @pl.when(jnp.logical_not(below[0]))
    def _():
        got_v[...] = layer
        got_p[...] = layer

    @pl.when(jnp.logical_not(above[0]))
    def _():
        got_u[...] = layer
        got_q[...] = layer

    @pl.when(jnp.logical_not(below[1]))
    def _():
        for k in range(3):
            bar[1 + k, :, TOP - 1 : TOP, :] = row
        pp[1, :, TOP - 1 : TOP, :] = row

    @pl.when(jnp.logical_not(above[1]))
    def _():
        bar[0, :, TOP + ys : TOP + ys + 1, :] = row
        for k in (XY, YY, YZ):
            qq[k, :, TOP + ys : TOP + ys + 1, :] = row

    @pl.when(jnp.logical_not(below[2]))
    def _():
        for k in range(3):
            bar[1 + k, 0, TOP : TOP + ys, :] = layer
        pp[2, 0, TOP : TOP + ys, :] = layer

    @pl.when(jnp.logical_not(above[2]))
    def _():
        bar[0, zs + 1, TOP : TOP + ys, :] = layer
        for k in (YZ, ZZ, XZ):
            qq[k, zs + 1, TOP : TOP + ys, :] = layer

    lane = lax.broadcasted_iota(jnp.int32, (8, xs), 1)
    sub = lax.broadcasted_iota(jnp.int32, (8, xs), 0)
    first_lane, last_lane = lane == 0, lane == xs - 1

    def factor(flag):
        return jnp.where(flag, jnp.float32(1), jnp.float32(0))

    up_x = jnp.where(last_lane, factor(above[0]), 1.0)
    lo_x = jnp.where(first_lane, factor(below[0]), 1.0)
    up_y_last = jnp.where(sub == 7, factor(above[1]), 1.0)
    lo_y_first = jnp.where(sub == 0, factor(below[1]), 1.0)

    def flush(later):
        for ref, at, value in later:
            ref[at + (slice(None),)] = value
        later.clear()

    def each(body):
        def turn(j, carry):
            body(2 * j)
            body(2 * j + 1)
            return carry

        lax.fori_loop(0, zs // 2, turn, 0)

    def sweep(body, moves, wanted):
        def turn(j, packed):
            one, two = list(packed[0]), list(packed[1])
            body(jnp.where(j == 0, 0, 2 * j - 1), one, two)
            body(jnp.where(j == 0, zs - 1, 2 * j), one, two)

            @pl.when(jnp.logical_and(wanted, j == 0))
            def _():
                start(moves)

            return tuple(one), tuple(two)

        return lax.fori_loop(0, zs // 2, turn, (nothing, nothing))

    def up_z(z):
        return factor(jnp.logical_or(z < zs - 1, above[2]))

    def lo_z(z):
        return factor(jnp.logical_or(z > 0, below[2]))

    def up_y(b, value):
        return up_y_last * value if b == blocks - 1 else value

    def lo_y(b, value):
        return lo_y_first * value if b == 0 else value

    def next_x(value):
        return jnp.where(last_lane, 0.0, pltpu.roll(value, xs - 1, 1))

    def prev_x(value):
        return jnp.where(first_lane, 0.0, pltpu.roll(value, 1, 1))

    def halo_next_x(got, k, z):
        return jnp.where(last_lane, pltpu.roll(got, xs - 1 - k * zs - z, 1), 0.0)

    def halo_prev_x(got, k, z):
        return jnp.where(first_lane, pltpu.roll(got, xs - 1 - k * zs - z, 1), 0.0)

    def next_y(ref, k, z, b, value):
        if b < blocks - 1:
            return ref[k, z + 1, rows(b, 1), :]
        return jnp.where(sub == 7, 0.0, pltpu.roll(value, 7, 0))

    def prev_y(ref, k, z, b, value):
        if b > 0:
            return ref[k, z + 1, rows(b, -1), :]
        return jnp.where(sub == 0, 0.0, pltpu.roll(value, 1, 0))

    def halo_next_y(ref, k, z, b):
        return jnp.where(sub == 7, ref[k, z + 1, rows(b, 1), :], 0.0)

    def halo_prev_y(ref, k, z, b):
        return jnp.where(sub == 0, ref[k, z + 1, rows(b, -1), :], 0.0)

    def next_z(ref, k, z, b):
        return factor(z < zs - 1) * ref[k, jnp.minimum(z + 2, zs), rows(b), :]

    def prev_z(ref, k, z, b):
        return factor(z > 0) * ref[k, jnp.maximum(z, 1), rows(b), :]

    def pack_first(packed, value, k, z):
        return jnp.where(lane == k * zs + z, pltpu.roll(value, k * zs + z, 1), packed)

    def pack_last(packed, value, k, z):
        return jnp.where(lane == k * zs + z + 1, pltpu.roll(value, k * zs + z + 2, 1), packed)

    def down(src, dst, i, k):
        return (
            pltpu.make_async_remote_copy(
                src_ref=src, dst_ref=dst, send_sem=send_sem.at[k], recv_sem=recv_sem.at[k],
                device_id={AXES[i]: place[i] - 1}, device_id_type=MESH,
            ),
            below[i],
            above[i],
        )

    def up(src, dst, i, k):
        return (
            pltpu.make_async_remote_copy(
                src_ref=src, dst_ref=dst, send_sem=send_sem.at[k], recv_sem=recv_sem.at[k],
                device_id={AXES[i]: place[i] + 1}, device_id_type=MESH,
            ),
            above[i],
            below[i],
        )

    comps = pl.ds(1, 3)
    primal_moves = [
        up(bar.at[comps, zs, mid_y], bar.at[comps, 0, mid_y], 2, 0),
        down(bar.at[0, 1, mid_y], bar.at[0, zs + 1, mid_y], 2, 1),
        up(bar.at[comps, mid_z, TOP + ys - 1], bar.at[comps, mid_z, TOP - 1], 1, 2),
        down(bar.at[0, mid_z, TOP], bar.at[0, mid_z, TOP + ys], 1, 3),
        up(send_v, got_v, 0, 4),
        down(send_u, got_u, 0, 5),
    ]
    dual_moves = [
        down(qq.at[pl.ds(YZ, 3), 1, mid_y], qq.at[pl.ds(YZ, 3), zs + 1, mid_y], 2, 6),
        up(pp.at[2, zs, mid_y], pp.at[2, 0, mid_y], 2, 7),
        down(qq.at[pl.ds(XY, 3), mid_z, TOP], qq.at[pl.ds(XY, 3), mid_z, TOP + ys], 1, 8),
        up(pp.at[1, mid_z, TOP + ys - 1], pp.at[1, mid_z, TOP - 1], 1, 9),
        down(send_q, got_q, 0, 10),
        up(send_p, got_p, 0, 11),
    ]

    def start(moves):
        for copy, goes, comes in moves:
            @pl.when(goes)
            def _():
                copy.start()

    def finish(moves):
        for copy, goes, comes in moves:
            @pl.when(goes)
            def _():
                copy.wait_send()

            @pl.when(comes)
            def _():
                copy.wait_recv()

    empty = jnp.zeros((8, xs), jnp.float32)

    def rows(b, by=0):
        return pl.ds(TOP + 8 * b + by, 8)

    def store_packed(ref, packed):
        for b in range(blocks):
            ref[pl.ds(8 * b, 8), :] = packed[b]

    for load in loads[:2]:
        load.wait()

    def first_faces(z, packed):
        first, last = list(packed[0]), list(packed[1])
        for b in range(blocks):
            first[b] = pack_first(first[b], bar[0, z + 1, rows(b), :], 0, z)
            for k in range(3):
                last[b] = pack_last(last[b], bar[1 + k, z + 1, rows(b), :], k, z)
        return tuple(first), tuple(last)

    nothing = (empty,) * blocks
    first, last = lax.fori_loop(0, zs, first_faces, (nothing, nothing))
    store_packed(send_u, first)
    store_packed(send_v, last)
    pl.semaphore_wait(barrier, peers)
    start(primal_moves)

    for load in loads[2:]:
        load.wait()

    def prepare(z, carry):
        weight = TAU * gain[z]
        inverse = 1.0 / (1.0 + weight)
        gain[z] = inverse
        offset[z] = weight * offset[z] * inverse
        u_out[z] = bar[0, z + 1, mid_y, :]
        for k in range(3):
            v_out[k, z] = bar[1 + k, z + 1, mid_y, :]
        return carry

    lax.fori_loop(0, zs, prepare, 0)

    def iteration(step, carry):
        more = step < ITERS - 1

        def dual_inside(z):
            later = []
            z_up, z_lo = up_z(z), lo_z(z)
            for b in range(blocks):
                r = rows(b)
                u = bar[0, z + 1, r, :]
                v = [bar[1 + k, z + 1, r, :] for k in range(3)]
                slopes = (
                    next_x(u) - up_x * u,
                    next_y(bar, 0, z, b, u) - up_y(b, u),
                    next_z(bar, 0, z, b) - z_up * u,
                )
                for k in range(3):
                    later.append((pp, (k, z + 1, r), pp[k, z + 1, r, :] + SIGMA * (slopes[k] - v[k])))
                dx = [lo_x * v[k] - prev_x(v[k]) for k in range(3)]
                dy = [lo_y(b, v[k]) - prev_y(bar, 1 + k, z, b, v[k]) for k in range(3)]
                dz = [z_lo * v[k] - prev_z(bar, 1 + k, z, b) for k in range(3)]
                half = 0.5 * SIGMA
                for k, add in (
                    (XX, SIGMA * dx[0]), (YY, SIGMA * dy[1]), (ZZ, SIGMA * dz[2]),
                    (XY, half * (dy[0] + dx[1])), (XZ, half * (dz[0] + dx[2])),
                    (YZ, half * (dz[1] + dy[2])),
                ):
                    later.append((qq, (k, z + 1, r), qq[k, z + 1, r, :] + add))
            flush(later)

        each(dual_inside)
        finish(primal_moves)

        def dual(z, of_p, of_q):
            z_end, z_begin, half = SIGMA * factor(z == zs - 1), factor(z == 0), 0.5 * SIGMA
            later = []
            for b in range(blocks):
                r, here = rows(b), pl.ds(8 * b, 8)
                t = [pp[k, z + 1, r, :] for k in range(3)]
                t[0] = t[0] + SIGMA * halo_next_x(got_u[here, :], 0, z)
                if b == blocks - 1:
                    t[1] = t[1] + SIGMA * halo_next_y(bar, 0, z, b)
                t[2] = t[2] + z_end * bar[0, z + 2, r, :]
                size = t[0] * t[0] + t[1] * t[1] + t[2] * t[2]
                scale = jnp.minimum(1.0, ALPHA1 * lax.rsqrt(size))
                t = [scale * part for part in t]
                for k in range(3):
                    later.append((pp, (k, z + 1, r), t[k]))
                    later.append((p_out, (k, z, here), t[k]))
                of_p[b] = pack_last(of_p[b], t[0], 0, z)

                received = got_v[here, :]
                hx = [halo_prev_x(received, k, z) for k in range(3)]
                hz = [z_begin * bar[1 + k, z, r, :] for k in range(3)]
                s = [qq[k, z + 1, r, :] for k in range(6)]
                s[XX] = s[XX] - SIGMA * hx[0]
                s[ZZ] = s[ZZ] - SIGMA * hz[2]
                s[XZ] = s[XZ] - half * (hz[0] + hx[2])
                if b == 0:
                    hy = [halo_prev_y(bar, 1 + k, z, b) for k in range(3)]
                    s[YY] = s[YY] - SIGMA * hy[1]
                    s[XY] = s[XY] - half * (hy[0] + hx[1])
                    s[YZ] = s[YZ] - half * (hz[1] + hy[2])
                else:
                    s[XY] = s[XY] - half * hx[1]
                    s[YZ] = s[YZ] - half * hz[1]
                size = (s[XX] * s[XX] + s[YY] * s[YY] + s[ZZ] * s[ZZ]) + 2.0 * (
                    s[XY] * s[XY] + s[XZ] * s[XZ] + s[YZ] * s[YZ]
                )
                scale = jnp.minimum(1.0, ALPHA0 * lax.rsqrt(size))
                s = [scale * part for part in s]
                for k in range(6):
                    later.append((qq, (k, z + 1, r), s[k]))
                    later.append((q_out, (Q_FROM[k], z, here), s[k]))
                for k, part in enumerate((XX, XY, XZ)):
                    of_q[b] = pack_first(of_q[b], s[part], k, z)
            flush(later)

        of_p, of_q = sweep(dual, dual_moves[:2], True)
        store_packed(send_p, of_p)
        store_packed(send_q, of_q)
        start(dual_moves[2:])

        parts_of = ((XX, XY, XZ), (XY, YY, YZ), (XZ, YZ, ZZ))

        def primal_inside(z):
            later = []
            z_up, z_lo = up_z(z), lo_z(z)
            for b in range(blocks):
                r, here = rows(b), pl.ds(8 * b, 8)
                p = [pp[k, z + 1, r, :] for k in range(3)]
                div = (
                    (up_x * p[0] - prev_x(p[0]))
                    + (up_y(b, p[1]) - prev_y(pp, 1, z, b, p[1]))
                    + (z_up * p[2] - prev_z(pp, 2, z, b))
                )
                new = (u_out[z, here, :] + TAU * div) * gain[z, here, :] + offset[z, here, :]
                later.append((partial, (0, z, here), new))
                q = [qq[k, z + 1, r, :] for k in range(6)]
                for k, (ax, ay, az) in enumerate(parts_of):
                    div2 = (
                        (next_x(q[ax]) - lo_x * q[ax])
                        + (next_y(qq, ay, z, b, q[ay]) - lo_y(b, q[ay]))
                        + (next_z(qq, az, z, b) - z_lo * q[az])
                    )
                    new = v_out[k, z, here, :] + TAU * (p[k] + div2)
                    later.append((partial, (1 + k, z, here), new))
            flush(later)

        each(primal_inside)
        finish(dual_moves)

        def primal(z, of_u, of_v):
            later = []
            z_end, z_begin = factor(z == zs - 1), factor(z == 0)
            for b in range(blocks):
                r, here = rows(b), pl.ds(8 * b, 8)
                received = got_q[here, :]
                for k, (ax, ay, az) in enumerate(parts_of):
                    halo = halo_next_x(received, k, z) + z_end * qq[az, z + 2, r, :]
                    if b == blocks - 1:
                        halo = halo + halo_next_y(qq, ay, z, b)
                    old = v_out[k, z, here, :]
                    new = partial[1 + k, z, here, :] + TAU * halo
                    later.append((v_out, (k, z, here), new))
                    ahead = 2.0 * new - old
                    later.append((bar, (1 + k, z + 1, r), ahead))
                    of_v[b] = pack_last(of_v[b], ahead, k, z)
                halo = halo_prev_x(got_p[here, :], 0, z) + z_begin * pp[2, z, r, :]
                if b == 0:
                    halo = halo + halo_prev_y(pp, 1, z, b)
                old = u_out[z, here, :]
                new = partial[0, z, here, :] - (TAU * halo) * gain[z, here, :]
                later.append((u_out, (z, here), new))
                ahead = 2.0 * new - old
                later.append((bar, (0, z + 1, r), ahead))
                of_u[b] = pack_first(of_u[b], ahead, 0, z)
            flush(later)

        of_u, of_v = sweep(primal, primal_moves[:2], more)

        @pl.when(more)
        def _():
            store_packed(send_u, of_u)
            store_packed(send_v, of_v)
            start(primal_moves[2:])

        return carry

    lax.fori_loop(0, ITERS, iteration, 0)


def copy_out(u_in, v_in, p_in, q_in, u_out, v_out, p_out, q_out, sems):
    pairs = ((q_in, q_out), (p_in, p_out), (v_in, v_out), (u_in, u_out))
    copies = [pltpu.make_async_copy(a, b, sems.at[i]) for i, (a, b) in enumerate(pairs)]
    for copy in copies:
        copy.start()
    for copy in copies:
        copy.wait()


def per_device(noisy_image, fidelity, primal_u, primal_v, dual_p, dual_q):
    zs, ys, xs = primal_u.shape
    assert xs == 128 and ys % 8 == 0 and zs % 2 == 0 and 3 * zs < xs
    f32 = jnp.float32
    padded = (zs + 2, ys + 2 * TOP, xs)
    face = pltpu.VMEM((ys, xs), f32)
    results = pl.pallas_call(
        kernel,
        out_shape=tuple(pltpu.VMEM(a.shape, f32) for a in (primal_u, primal_v, dual_p, dual_q)),
        in_specs=[pl.BlockSpec(memory_space=pl.ANY)] * 6,
        out_specs=tuple([pl.BlockSpec(memory_space=pltpu.VMEM)] * 4),
        scratch_shapes=[
            pltpu.VMEM((4,) + padded, f32),
            pltpu.VMEM((3,) + padded, f32),
            pltpu.VMEM((6,) + padded, f32),
            pltpu.VMEM((zs, ys, xs), f32),
            pltpu.VMEM((zs, ys, xs), f32),
            pltpu.VMEM((4, zs, ys, xs), f32),
        ]
        + [face] * 8
        + [
            pltpu.SemaphoreType.DMA((11,)),
            pltpu.SemaphoreType.DMA((12,)),
            pltpu.SemaphoreType.DMA((12,)),
        ],
        compiler_params=pltpu.CompilerParams(collective_id=0, has_side_effects=True),
        name="tgv",
    )(noisy_image, fidelity, primal_u, primal_v, dual_p, dual_q)
    return pl.pallas_call(
        copy_out,
        out_shape=tuple(jax.ShapeDtypeStruct(a.shape, f32) for a in results),
        in_specs=[pl.BlockSpec(memory_space=pltpu.VMEM)] * 4,
        out_specs=tuple([pl.BlockSpec(memory_space=pl.ANY)] * 4),
        scratch_shapes=[pltpu.SemaphoreType.DMA((4,))],
        name="out",
    )(*[pltpu.with_memory_space_constraint(r, pltpu.VMEM) for r in results])


def solution(mesh):
    scalar, stack = P("gz", "gy", "gx"), P(None, "gz", "gy", "gx")
    return jax.shard_map(
        per_device,
        mesh=mesh,
        in_specs=(scalar, scalar, scalar, stack, stack, stack),
        out_specs=(scalar, stack, stack, stack),
        check_vma=False,
    )
```

```python
import functools

import jax
import jax.numpy as jnp
from jax import lax
from jax.experimental import pallas as pl
from jax.experimental.pallas import tpu as pltpu
from jax.sharding import PartitionSpec as P

ITERS = 3
AXES = ("gx", "gy", "gz")
ALPHA1, ALPHA0, SIGMA, TAU = 0.5, 1.0, 0.2, 0.2
Q_FROM = (0, 3, 1, 5, 2, 4)
GROUP = 4
XX, XY, YY, YZ, ZZ, XZ = range(6)
MESH = pl.DeviceIdType.MESH
TOP = 8


def kernel(
    noisy_in, fid_in, u_in, v_in, p_in, q_in,
    u_out, v_out, p_out, q_out,
    bar, pp, qq, gain, offset, partial,
    send_u, send_v, send_p, send_q, got_u, got_v, got_p, got_q,
    load_sem, send_sem, recv_sem,
):
    zs, ys, xs = u_in.shape
    blocks = ys // 8
    place = [lax.axis_index(a) for a in AXES]
    count = [lax.axis_size(a) for a in AXES]
    below = [place[i] > 0 for i in range(3)]
    above = [place[i] < count[i] - 1 for i in range(3)]

    peers = sum(there.astype(jnp.int32) for there in below + above)

    barrier = pltpu.get_barrier_semaphore()
    for i in range(3):
        for there, by in ((below[i], -1), (above[i], 1)):
            @pl.when(there)
            def _():
                pl.semaphore_signal(
                    barrier, inc=1, device_id={AXES[i]: place[i] + by}, device_id_type=MESH
                )

    mid_z, mid_y = pl.ds(1, zs), pl.ds(TOP, ys)
    loads = [
        pltpu.make_async_copy(u_in, bar.at[0, mid_z, mid_y], load_sem.at[0]),
        pltpu.make_async_copy(v_in, bar.at[pl.ds(1, 3), mid_z, mid_y], load_sem.at[1]),
        pltpu.make_async_copy(p_in, pp.at[:, mid_z, mid_y], load_sem.at[2]),
        pltpu.make_async_copy(noisy_in, offset, load_sem.at[3]),
        pltpu.make_async_copy(fid_in, gain, load_sem.at[4]),
    ] + [
        pltpu.make_async_copy(q_in.at[Q_FROM[k]], qq.at[k, mid_z, mid_y], load_sem.at[5 + k])
        for k in range(6)
    ]
    for load in loads:
        load.start()

    row = jnp.zeros((zs + 2, 1, xs), jnp.float32)
    layer = jnp.zeros((ys, xs), jnp.float32)

    @pl.when(jnp.logical_not(below[0]))
    def _():
        got_v[...] = layer
        got_p[...] = layer

    @pl.when(jnp.logical_not(above[0]))
    def _():
        got_u[...] = layer
        got_q[...] = layer

    @pl.when(jnp.logical_not(below[1]))
    def _():
        for k in range(3):
            bar[1 + k, :, TOP - 1 : TOP, :] = row
        pp[1, :, TOP - 1 : TOP, :] = row

    @pl.when(jnp.logical_not(above[1]))
    def _():
        bar[0, :, TOP + ys : TOP + ys + 1, :] = row
        for k in (XY, YY, YZ):
            qq[k, :, TOP + ys : TOP + ys + 1, :] = row

    @pl.when(jnp.logical_not(below[2]))
    def _():
        for k in range(3):
            bar[1 + k, 0, TOP : TOP + ys, :] = layer
        pp[2, 0, TOP : TOP + ys, :] = layer

    @pl.when(jnp.logical_not(above[2]))
    def _():
        bar[0, zs + 1, TOP : TOP + ys, :] = layer
        for k in (YZ, ZZ, XZ):
            qq[k, zs + 1, TOP : TOP + ys, :] = layer

    lane = lax.broadcasted_iota(jnp.int32, (8, xs), 1)
    sub = lax.broadcasted_iota(jnp.int32, (8, xs), 0)
    first_lane, last_lane = lane == 0, lane == xs - 1

    def factor(flag):
        return jnp.where(flag, jnp.float32(1), jnp.float32(0))

    up_x = jnp.where(last_lane, factor(above[0]), 1.0)
    lo_x = jnp.where(first_lane, factor(below[0]), 1.0)
    up_y_last = jnp.where(sub == 7, factor(above[1]), 1.0)
    lo_y_first = jnp.where(sub == 0, factor(below[1]), 1.0)

    def flush(later):
        for ref, at, value in later:
            ref[at + (slice(None),)] = value
        later.clear()

    def each(body):
        def turn(j, carry):
            body(2 * j)
            body(2 * j + 1)
            return carry

        lax.fori_loop(0, zs // 2, turn, 0)

    def sweep(body, moves, wanted):
        def turn(j, packed):
            one, two = list(packed[0]), list(packed[1])
            body(jnp.where(j == 0, 0, 2 * j - 1), one, two)
            body(jnp.where(j == 0, zs - 1, 2 * j), one, two)

            @pl.when(jnp.logical_and(wanted, j == 0))
            def _():
                start(moves)

            return tuple(one), tuple(two)

        return lax.fori_loop(0, zs // 2, turn, (nothing, nothing))

    def up_z(z):
        return factor(jnp.logical_or(z < zs - 1, above[2]))

    def lo_z(z):
        return factor(jnp.logical_or(z > 0, below[2]))

    def up_y(b, value):
        return up_y_last * value if b == blocks - 1 else value

    def lo_y(b, value):
        return lo_y_first * value if b == 0 else value

    def next_x(value):
        return jnp.where(last_lane, 0.0, pltpu.roll(value, xs - 1, 1))

    def prev_x(value):
        return jnp.where(first_lane, 0.0, pltpu.roll(value, 1, 1))

    def halo_next_x(got, k, z):
        return jnp.where(last_lane, pltpu.roll(got, xs - 1 - k * zs - z, 1), 0.0)

    def halo_prev_x(got, k, z):
        return jnp.where(first_lane, pltpu.roll(got, xs - 1 - k * zs - z, 1), 0.0)

    def next_y(ref, k, z, b, value):
        if b < blocks - 1:
            return ref[k, z + 1, rows(b, 1), :]
        return jnp.where(sub == 7, 0.0, pltpu.roll(value, 7, 0))

    def prev_y(ref, k, z, b, value):
        if b > 0:
            return ref[k, z + 1, rows(b, -1), :]
        return jnp.where(sub == 0, 0.0, pltpu.roll(value, 1, 0))

    def halo_next_y(ref, k, z, b):
        return jnp.where(sub == 7, ref[k, z + 1, rows(b, 1), :], 0.0)

    def halo_prev_y(ref, k, z, b):
        return jnp.where(sub == 0, ref[k, z + 1, rows(b, -1), :], 0.0)

    def next_z(ref, k, z, b):
        return factor(z < zs - 1) * ref[k, jnp.minimum(z + 2, zs), rows(b), :]

    def prev_z(ref, k, z, b):
        return factor(z > 0) * ref[k, jnp.maximum(z, 1), rows(b), :]

    def pack_first(packed, value, k, z):
        return jnp.where(lane == k * zs + z, pltpu.roll(value, k * zs + z, 1), packed)

    def pack_last(packed, value, k, z):
        return jnp.where(lane == k * zs + z + 1, pltpu.roll(value, k * zs + z + 2, 1), packed)

    def down(src, dst, i, k):
        return (
            pltpu.make_async_remote_copy(
                src_ref=src, dst_ref=dst, send_sem=send_sem.at[k], recv_sem=recv_sem.at[k],
                device_id={AXES[i]: place[i] - 1}, device_id_type=MESH,
            ),
            below[i],
            above[i],
        )

    def up(src, dst, i, k):
        return (
            pltpu.make_async_remote_copy(
                src_ref=src, dst_ref=dst, send_sem=send_sem.at[k], recv_sem=recv_sem.at[k],
                device_id={AXES[i]: place[i] + 1}, device_id_type=MESH,
            ),
            above[i],
            below[i],
        )

    comps = pl.ds(1, 3)
    primal_moves = [
        up(bar.at[comps, zs, mid_y], bar.at[comps, 0, mid_y], 2, 0),
        down(bar.at[0, 1, mid_y], bar.at[0, zs + 1, mid_y], 2, 1),
        up(bar.at[comps, mid_z, TOP + ys - 1], bar.at[comps, mid_z, TOP - 1], 1, 2),
        down(bar.at[0, mid_z, TOP], bar.at[0, mid_z, TOP + ys], 1, 3),
        up(send_v, got_v, 0, 4),
        down(send_u, got_u, 0, 5),
    ]
    dual_moves = [
        down(qq.at[pl.ds(YZ, 3), 1, mid_y], qq.at[pl.ds(YZ, 3), zs + 1, mid_y], 2, 6),
        up(pp.at[2, zs, mid_y], pp.at[2, 0, mid_y], 2, 7),
        down(qq.at[pl.ds(XY, 3), mid_z, TOP], qq.at[pl.ds(XY, 3), mid_z, TOP + ys], 1, 8),
        up(pp.at[1, mid_z, TOP + ys - 1], pp.at[1, mid_z, TOP - 1], 1, 9),
        down(send_q, got_q, 0, 10),
        up(send_p, got_p, 0, 11),
    ]

    def start(moves):
        for copy, goes, comes in moves:
            @pl.when(goes)
            def _():
                copy.start()

    def finish(moves):
        for copy, goes, comes in moves:
            @pl.when(goes)
            def _():
                copy.wait_send()

            @pl.when(comes)
            def _():
                copy.wait_recv()

    empty = jnp.zeros((8, xs), jnp.float32)

    def rows(b, by=0):
        return pl.ds(TOP + 8 * b + by, 8)

    def store_packed(ref, packed):
        for b in range(blocks):
            ref[pl.ds(8 * b, 8), :] = packed[b]

    for load in loads[:2]:
        load.wait()
    pl.semaphore_wait(barrier, peers)
    start(primal_moves[:4])

    def first_faces(z, packed):
        first, last = list(packed[0]), list(packed[1])
        for b in range(blocks):
            first[b] = pack_first(first[b], bar[0, z + 1, rows(b), :], 0, z)
            for k in range(3):
                last[b] = pack_last(last[b], bar[1 + k, z + 1, rows(b), :], k, z)
        return tuple(first), tuple(last)

    nothing = (empty,) * blocks
    first, last = lax.fori_loop(0, zs, first_faces, (nothing, nothing))
    store_packed(send_u, first)
    store_packed(send_v, last)
    start(primal_moves[4:])

    for load in loads[2:]:
        load.wait()

    def prepare(z, carry):
        weight = TAU * gain[z]
        inverse = 1.0 / (1.0 + weight)
        gain[z] = inverse
        offset[z] = weight * offset[z] * inverse
        u_out[z] = bar[0, z + 1, mid_y, :]
        for k in range(3):
            v_out[k, z] = bar[1 + k, z + 1, mid_y, :]
        return carry

    lax.fori_loop(0, zs, prepare, 0)

    def iteration(step, carry):
        more = step < ITERS - 1

        def dual_inside(z):
            later = []
            z_up, z_lo = up_z(z), lo_z(z)
            for b in range(blocks):
                r = rows(b)
                u = bar[0, z + 1, r, :]
                v = [bar[1 + k, z + 1, r, :] for k in range(3)]
                slopes = (
                    next_x(u) - up_x * u,
                    next_y(bar, 0, z, b, u) - up_y(b, u),
                    next_z(bar, 0, z, b) - z_up * u,
                )
                for k in range(3):
                    later.append((pp, (k, z + 1, r), pp[k, z + 1, r, :] + SIGMA * (slopes[k] - v[k])))
                dx = [lo_x * v[k] - prev_x(v[k]) for k in range(3)]
                dy = [lo_y(b, v[k]) - prev_y(bar, 1 + k, z, b, v[k]) for k in range(3)]
                dz = [z_lo * v[k] - prev_z(bar, 1 + k, z, b) for k in range(3)]
                half = 0.5 * SIGMA
                for k, add in (
                    (XX, SIGMA * dx[0]), (YY, SIGMA * dy[1]), (ZZ, SIGMA * dz[2]),
                    (XY, half * (dy[0] + dx[1])), (XZ, half * (dz[0] + dx[2])),
                    (YZ, half * (dz[1] + dy[2])),
                ):
                    later.append((qq, (k, z + 1, r), qq[k, z + 1, r, :] + add))
            flush(later)

        each(dual_inside)
        finish(primal_moves)

        def dual(z, of_p, of_q):
            z_end, z_begin, half = SIGMA * factor(z == zs - 1), factor(z == 0), 0.5 * SIGMA
            later = []
            for b in range(blocks):
                r, here = rows(b), pl.ds(8 * b, 8)
                t = [pp[k, z + 1, r, :] for k in range(3)]
                t[0] = t[0] + SIGMA * halo_next_x(got_u[here, :], 0, z)
                if b == blocks - 1:
                    t[1] = t[1] + SIGMA * halo_next_y(bar, 0, z, b)
                t[2] = t[2] + z_end * bar[0, z + 2, r, :]
                size = t[0] * t[0] + t[1] * t[1] + t[2] * t[2]
                scale = jnp.minimum(1.0, ALPHA1 * lax.rsqrt(size))
                t = [scale * part for part in t]
                for k in range(3):
                    later.append((pp, (k, z + 1, r), t[k]))
                    later.append((p_out, (k, z, here), t[k]))
                of_p[b] = pack_last(of_p[b], t[0], 0, z)

                received = got_v[here, :]
                hx = [halo_prev_x(received, k, z) for k in range(3)]
                hz = [z_begin * bar[1 + k, z, r, :] for k in range(3)]
                s = [qq[k, z + 1, r, :] for k in range(6)]
                s[XX] = s[XX] - SIGMA * hx[0]
                s[ZZ] = s[ZZ] - SIGMA * hz[2]
                s[XZ] = s[XZ] - half * (hz[0] + hx[2])
                if b == 0:
                    hy = [halo_prev_y(bar, 1 + k, z, b) for k in range(3)]
                    s[YY] = s[YY] - SIGMA * hy[1]
                    s[XY] = s[XY] - half * (hy[0] + hx[1])
                    s[YZ] = s[YZ] - half * (hz[1] + hy[2])
                else:
                    s[XY] = s[XY] - half * hx[1]
                    s[YZ] = s[YZ] - half * hz[1]
                size = (s[XX] * s[XX] + s[YY] * s[YY] + s[ZZ] * s[ZZ]) + 2.0 * (
                    s[XY] * s[XY] + s[XZ] * s[XZ] + s[YZ] * s[YZ]
                )
                scale = jnp.minimum(1.0, ALPHA0 * lax.rsqrt(size))
                s = [scale * part for part in s]
                for k in range(6):
                    later.append((qq, (k, z + 1, r), s[k]))
                    later.append((q_out, (Q_FROM[k], z, here), s[k]))
                for k, part in enumerate((XX, XY, XZ)):
                    of_q[b] = pack_first(of_q[b], s[part], k, z)
            flush(later)

        of_p, of_q = sweep(dual, dual_moves[:2], True)
        store_packed(send_p, of_p)
        store_packed(send_q, of_q)
        start(dual_moves[2:])

        parts_of = ((XX, XY, XZ), (XY, YY, YZ), (XZ, YZ, ZZ))

        def primal_inside(z):
            later = []
            z_up, z_lo = up_z(z), lo_z(z)
            for b in range(blocks):
                r, here = rows(b), pl.ds(8 * b, 8)
                p = [pp[k, z + 1, r, :] for k in range(3)]
                div = (
                    (up_x * p[0] - prev_x(p[0]))
                    + (up_y(b, p[1]) - prev_y(pp, 1, z, b, p[1]))
                    + (z_up * p[2] - prev_z(pp, 2, z, b))
                )
                new = (u_out[z, here, :] + TAU * div) * gain[z, here, :] + offset[z, here, :]
                later.append((partial, (0, z, here), new))
                q = [qq[k, z + 1, r, :] for k in range(6)]
                for k, (ax, ay, az) in enumerate(parts_of):
                    div2 = (
                        (next_x(q[ax]) - lo_x * q[ax])
                        + (next_y(qq, ay, z, b, q[ay]) - lo_y(b, q[ay]))
                        + (next_z(qq, az, z, b) - z_lo * q[az])
                    )
                    new = v_out[k, z, here, :] + TAU * (p[k] + div2)
                    later.append((partial, (1 + k, z, here), new))
            flush(later)

        each(primal_inside)
        finish(dual_moves)

        def primal(z, of_u, of_v):
            later = []
            z_end, z_begin = factor(z == zs - 1), factor(z == 0)
            for b in range(blocks):
                r, here = rows(b), pl.ds(8 * b, 8)
                received = got_q[here, :]
                for k, (ax, ay, az) in enumerate(parts_of):
                    halo = halo_next_x(received, k, z) + z_end * qq[az, z + 2, r, :]
                    if b == blocks - 1:
                        halo = halo + halo_next_y(qq, ay, z, b)
                    old = v_out[k, z, here, :]
                    new = partial[1 + k, z, here, :] + TAU * halo
                    later.append((v_out, (k, z, here), new))
                    ahead = 2.0 * new - old
                    later.append((bar, (1 + k, z + 1, r), ahead))
                    of_v[b] = pack_last(of_v[b], ahead, k, z)
                halo = halo_prev_x(got_p[here, :], 0, z) + z_begin * pp[2, z, r, :]
                if b == 0:
                    halo = halo + halo_prev_y(pp, 1, z, b)
                old = u_out[z, here, :]
                new = partial[0, z, here, :] - (TAU * halo) * gain[z, here, :]
                later.append((u_out, (z, here), new))
                ahead = 2.0 * new - old
                later.append((bar, (0, z + 1, r), ahead))
                of_u[b] = pack_first(of_u[b], ahead, 0, z)
            flush(later)

        of_u, of_v = sweep(primal, primal_moves[:2], more)

        @pl.when(more)
        def _():
            store_packed(send_u, of_u)
            store_packed(send_v, of_v)
            start(primal_moves[2:])

        return carry

    lax.fori_loop(0, ITERS, iteration, 0)


def copy_out(u_in, v_in, p_in, q_in, u_out, v_out, p_out, q_out, sems):
    pairs = ((q_in, q_out), (p_in, p_out), (v_in, v_out), (u_in, u_out))
    copies = [pltpu.make_async_copy(a, b, sems.at[i]) for i, (a, b) in enumerate(pairs)]
    for copy in copies:
        copy.start()
    for copy in copies:
        copy.wait()


def per_device(noisy_image, fidelity, primal_u, primal_v, dual_p, dual_q):
    zs, ys, xs = primal_u.shape
    assert xs == 128 and ys % 8 == 0 and zs % 2 == 0 and 3 * zs < xs
    f32 = jnp.float32
    padded = (zs + 2, ys + 2 * TOP, xs)
    face = pltpu.VMEM((ys, xs), f32)
    results = pl.pallas_call(
        kernel,
        out_shape=tuple(pltpu.VMEM(a.shape, f32) for a in (primal_u, primal_v, dual_p, dual_q)),
        in_specs=[pl.BlockSpec(memory_space=pl.ANY)] * 6,
        out_specs=tuple([pl.BlockSpec(memory_space=pltpu.VMEM)] * 4),
        scratch_shapes=[
            pltpu.VMEM((4,) + padded, f32),
            pltpu.VMEM((3,) + padded, f32),
            pltpu.VMEM((6,) + padded, f32),
            pltpu.VMEM((zs, ys, xs), f32),
            pltpu.VMEM((zs, ys, xs), f32),
            pltpu.VMEM((4, zs, ys, xs), f32),
        ]
        + [face] * 8
        + [
            pltpu.SemaphoreType.DMA((11,)),
            pltpu.SemaphoreType.DMA((12,)),
            pltpu.SemaphoreType.DMA((12,)),
        ],
        compiler_params=pltpu.CompilerParams(collective_id=0, has_side_effects=True),
        name="tgv",
    )(noisy_image, fidelity, primal_u, primal_v, dual_p, dual_q)
    return pl.pallas_call(
        copy_out,
        out_shape=tuple(jax.ShapeDtypeStruct(a.shape, f32) for a in results),
        in_specs=[pl.BlockSpec(memory_space=pltpu.VMEM)] * 4,
        out_specs=tuple([pl.BlockSpec(memory_space=pl.ANY)] * 4),
        scratch_shapes=[pltpu.SemaphoreType.DMA((4,))],
        name="out",
    )(*[pltpu.with_memory_space_constraint(r, pltpu.VMEM) for r in results])


def solution(mesh):
    scalar, stack = P("gz", "gy", "gx"), P(None, "gz", "gy", "gx")
    return jax.shard_map(
        per_device,
        mesh=mesh,
        in_specs=(scalar, scalar, scalar, stack, stack, stack),
        out_specs=(scalar, stack, stack, stack),
        check_vma=False,
    )
```
